32 devices in a mesh: group: 2 (over y), seq: 16 (over z, x, core).
Axes of the slice: x: 2, y: 2, z: 4, core: 2. Of those that a mesh axis runs over, the one named last changes fastest.
Arguments:
- query_frames: bfloat16 [16384, 4096], P(('group', 'seq')), parts along dimension 0, may hold values from -5 to 5
- key_frames: bfloat16 [16384, 512], P(('group', 'seq')), parts along dimension 0, may hold values from -5 to 5
- value_frames: bfloat16 [16384, 512], P(('group', 'seq')), parts along dimension 0, may hold values from -6 to 6
- token_counts: int32 [32], P(('group', 'seq')), parts along dimension 0, may hold values from 1 to 511, as said below
- segments: int32 [8192], P('group'), parts along dimension 0, may hold values from 0 to 7, as said below
Outputs:
- attended: bfloat16 [8192, 4096], P(('group', 'seq')), parts along dimension 0
The draws below stay inside these ranges and needn't reach their ends.
There are 2 independent parts, one for each index of `group`. The reference program is written for one: setup_inputs(seed, part) draws one part's arguments, and reference() takes and returns one part's arrays. A program takes and returns all parts, laid end to end along the dimension named above; each array names one. Nothing has to cross between parts.
Inputs may be any that keep to these rules, and one draw needn't show every extreme that they name: `token_counts`: entry d belongs to device d of seq. The counts before entry d sum to a number from d * 256 to d * 256 + 255, and all counts sum to 4096. `segments`: sequence numbers never fall along the positions and each of 0 to 7 appears; each packed sequence covers 1 to 1024 consecutive positions, one exactly 1024; the first covers more than 256.
All inputs are finite; a program needn't handle non-finite values.
Results may differ from the reference program's by a relative error of at most 0.013.
Values may be sent and summed in bfloat16 or wider, within the bound.
A program may use at most 64 MiB of HBM per device.

```python
import math
import jax
import jax.numpy as jnp
from jax import lax

Q_HEADS = 32
KV_HEADS = 4
HEAD_DIM = 128
SPAN = 256
WINDOW = 5
CYCLE = 16
FRAME_CAP = 512
FRAME_ROWS = 8192
SEQ_LEN = 4096
CLIPS = 8
QW = 4096
KW = 512


def draw_query_frames(key, part):
    groups = Q_HEADS // KV_HEADS
    shape = (FRAME_ROWS, KV_HEADS, groups, HEAD_DIM)
    values = jnp.clip(jax.random.normal(jax.random.fold_in(key, 1), shape, jnp.float32), -5.0, 5.0)
    return values.reshape(FRAME_ROWS, Q_HEADS * HEAD_DIM).astype(jnp.bfloat16)


def draw_key_frames(key, part):
    shape = (FRAME_ROWS, KV_HEADS, HEAD_DIM)
    values = jnp.clip(jax.random.normal(jax.random.fold_in(key, 2), shape, jnp.float32), -5.0, 5.0)
    return values.reshape(FRAME_ROWS, KV_HEADS * HEAD_DIM).astype(jnp.bfloat16)


def draw_token_counts(key, part):
    places = jnp.arange(CYCLE + 1, dtype=jnp.int32)
    leads = jax.random.randint(jax.random.fold_in(key, 21), (CYCLE + 1,), 0, SPAN, dtype=jnp.int32)
    widest = jax.random.randint(jax.random.fold_in(key, 22), (), 0, CYCLE - 1, dtype=jnp.int32)
    leads = jnp.where(places == widest, 0, leads)
    leads = jnp.where(places == widest + 1, SPAN - 1, leads)
    leads = jnp.where((places == 0) | (places == CYCLE), 0, leads)
    return (SPAN + leads[1:] - leads[:-1]).astype(jnp.int32)


def draw_segments(key, part):
    marks = jnp.arange(CLIPS + 1, dtype=jnp.int32)
    shifts = jax.random.randint(jax.random.fold_in(key, 31), (CLIPS + 1,), 1 - SPAN, SPAN, dtype=jnp.int32)
    firsts = jax.random.randint(jax.random.fold_in(key, 32), (), 0, SPAN, dtype=jnp.int32)
    shifts = jnp.where(marks == 1, firsts, shifts)
    widest = jax.random.randint(jax.random.fold_in(key, 33), (), 3, CLIPS, dtype=jnp.int32)
    shifts = jnp.where(marks == widest - 1, -SPAN, shifts)
    shifts = jnp.where(marks == widest, SPAN, shifts)
    shifts = jnp.where((marks == 0) | (marks == CLIPS), 0, shifts)
    bounds = (2 * SPAN * marks + shifts)[1:CLIPS]
    places = jnp.arange(SEQ_LEN, dtype=jnp.int32)
    return jnp.sum((places[:, None] >= bounds[None, :]).astype(jnp.int32), axis=1).astype(jnp.int32)


def block_levels(rng, dims, cuts, smallest, top_value):
    def one(position, parts):
        draws = jax.random.uniform(jax.random.fold_in(jax.random.fold_in(rng, 6), position), (parts,), jnp.float32, smallest / len(cuts), top_value / len(cuts))
        return jnp.repeat(jnp.exp(draws), dims[position] // parts).reshape((-1,) + (1,) * (len(dims) - position - 1))

    factor_of = one(*cuts[0])
    for cut in cuts[1:]:
        factor_of = factor_of * one(*cut)
    return factor_of


def normal_values(own_key, shape, width, bound, shards=(), kind=jnp.bfloat16):
    drawn = width * jax.random.normal(own_key, shape, jnp.float32)
    if shards:
        drawn = drawn * block_levels(own_key, shape, shards, -0.22, 0.18)
    return jnp.clip(drawn, -bound, bound).astype(kind)


def setup_inputs(seed: int = 0, part: int = 0) -> dict:
    streams_of = jax.random.split(jax.random.key(seed), 6)
    part_keys = jax.random.split(jax.random.fold_in(streams_of[5], part), 6)
    return {
        "query_frames": draw_query_frames(jax.random.fold_in(jax.random.fold_in(streams_of[5], part), 71), part),
        "key_frames": draw_key_frames(jax.random.fold_in(jax.random.fold_in(streams_of[5], part), 71), part),
        "value_frames": normal_values(part_keys[2], (FRAME_ROWS, KW), 1.0, 6.0, ((0, 16),)),
        "token_counts": draw_token_counts(jax.random.fold_in(jax.random.fold_in(streams_of[5], part), 71), part),
        "segments": draw_segments(jax.random.fold_in(jax.random.fold_in(streams_of[5], part), 71), part),
    }


def reference(query_frames, key_frames, value_frames, token_counts, segments):
    counts = token_counts.astype(jnp.int32)
    offsets = (jnp.cumsum(counts) - counts).astype(jnp.int32)
    places = jnp.arange(SEQ_LEN, dtype=jnp.int32)
    owners = (jnp.searchsorted(offsets, places, side='right') - 1).astype(jnp.int32)
    source = (owners * FRAME_CAP + places - offsets[owners]).astype(jnp.int32)
    queries = query_frames[source]
    keys = key_frames[source]
    values = value_frames[source]
    margin = (WINDOW - 1) * SPAN
    keys_padded = jnp.concatenate([jnp.zeros((margin, KW), keys.dtype), keys], axis=0)
    values_padded = jnp.concatenate([jnp.zeros((margin, KW), values.dtype), values], axis=0)
    clips_padded = jnp.concatenate([jnp.full((margin,), -1, jnp.int32), segments.astype(jnp.int32)], axis=0)
    groups = Q_HEADS // KV_HEADS
    inverse_root = 1.0 / math.sqrt(HEAD_DIM)

    def one_block(block_number):
        first = (block_number * SPAN).astype(jnp.int32)
        query_block = lax.dynamic_slice_in_dim(queries, first, SPAN, 0).astype(jnp.float32).reshape(SPAN, KV_HEADS, groups, HEAD_DIM)
        key_block = lax.dynamic_slice_in_dim(keys_padded, first, WINDOW * SPAN, 0).astype(jnp.float32).reshape(WINDOW * SPAN, KV_HEADS, HEAD_DIM)
        value_block = lax.dynamic_slice_in_dim(values_padded, first, WINDOW * SPAN, 0).astype(jnp.float32).reshape(WINDOW * SPAN, KV_HEADS, HEAD_DIM)
        query_clip = lax.dynamic_slice_in_dim(segments.astype(jnp.int32), first, SPAN, 0)
        key_clip = lax.dynamic_slice_in_dim(clips_padded, first, WINDOW * SPAN, 0)
        query_place = first + jnp.arange(SPAN, dtype=jnp.int32)
        key_place = first - margin + jnp.arange(WINDOW * SPAN, dtype=jnp.int32)
        allowed = (key_place[None, :] <= query_place[:, None]) & (key_clip[None, :] == query_clip[:, None])
        scores = jnp.einsum('qhgd,khd->hgqk', query_block, key_block) * inverse_root
        masked = jnp.where(allowed, scores, -jnp.inf)
        highest = lax.optimization_barrier(jnp.max(masked, axis=-1, keepdims=True))
        weights = jnp.where(allowed, jnp.exp(masked - highest), 0.0)
        totals = lax.optimization_barrier(jnp.sum(weights, axis=-1))
        rounded = lax.optimization_barrier(weights.astype(jnp.bfloat16)).astype(jnp.float32)
        summed = jnp.einsum('hgqk,khd->qhgd', rounded, value_block)
        result = summed / jnp.transpose(totals, (2, 0, 1))[..., None]
        return result.reshape(SPAN, QW).astype(jnp.bfloat16)
    blocks = lax.map(one_block, jnp.arange(CYCLE, dtype=jnp.int32))
    return blocks.reshape(SEQ_LEN, QW)
```

```python
import functools
import math

import jax
import jax.numpy as jnp
from jax import lax
from jax.experimental import pallas as pl
from jax.experimental.pallas import tpu as pltpu
from jax.sharding import PartitionSpec as P

Q_HEADS = 32
KV_HEADS = 4
HEAD_DIM = 128
SPAN = 256
WINDOW = 5
CHUNK_HEADS = 4
CHUNK = CHUNK_HEADS * HEAD_DIM
CHUNKS = Q_HEADS // CHUNK_HEADS
EARLY = 2
KW = KV_HEADS * HEAD_DIM
LAST = WINDOW - 1
LOW = -(2.0**100)
BF16 = jnp.bfloat16
F32 = jnp.float32


def one_hot(rows, columns, shift):
    row = lax.broadcasted_iota(jnp.int32, (rows, columns), 0)
    column = lax.broadcasted_iota(jnp.int32, (rows, columns), 1)
    return jnp.where(column == row + shift, 1.0, 0.0).astype(BF16)


def kernel(
    n, count_ref, seg_ref, qf, kf, vf, out,
    counts, q_in, q_tail, q_got, kv_in, kv_tail, kv_got, window, keys_t, vals, causal, clips, o_buf,
    in_sem, kv_in_sem, out_sem, cnt_send, cnt_recv, tail_send, tail_recv, q_send, q_recv, kv_send, kv_recv,
):
    me = lax.axis_index("seq")
    core = lax.rem(me, 2)
    cap = kv_in.shape[0]

    kv_loads = [
        pltpu.make_async_copy(kf, kv_in.at[:, pl.ds(0, KW)], kv_in_sem.at[0]),
        pltpu.make_async_copy(vf, kv_in.at[:, pl.ds(KW, KW)], kv_in_sem.at[1]),
    ]
    q_loads = [
        pltpu.make_async_copy(qf.at[:, pl.ds(c * CHUNK, CHUNK)], q_in.at[c], in_sem.at[c])
        for c in range(CHUNKS)
    ]
    for load in kv_loads + q_loads:
        load.start()

    count = count_ref[0]
    counts[me] = jnp.full(counts.shape[1:], count, jnp.int32)

    for slot in range(LAST):
        @pl.when(me < LAST - slot)
        def _():
            window[slot] = jnp.zeros(window.shape[1:], BF16)

    @pl.when(me == 0)
    def _():
        kv_got[...] = jnp.zeros_like(kv_got)
        q_got[...] = jnp.zeros_like(q_got)

    barrier = pltpu.get_barrier_semaphore()

    @pl.loop(1, n)
    def _(step):
        pl.semaphore_signal(barrier, inc=1, device_id={"seq": lax.rem(me + step, n)})

    pl.semaphore_wait(barrier, n - 1)

    def remote(src, dst, send, recv, target):
        return pltpu.make_async_remote_copy(
            src_ref=src, dst_ref=dst, send_sem=send, recv_sem=recv, device_id={"seq": target}
        )

    def count_copy(sender, target):
        return remote(counts.at[sender], counts.at[sender], cnt_send.at[target], cnt_recv.at[sender], target)

    @pl.loop(me + 1, n)
    def _(target):
        count_copy(me, target).start()

    for load in kv_loads:
        load.wait()
    ending = one_hot(SPAN, cap, count - SPAN)
    kv_tail[...] = jnp.dot(ending, kv_in[...], preferred_element_type=F32).astype(BF16)

    def tail_of(c):
        q_loads[c].wait()
        q_tail[c] = jnp.dot(ending, q_in[c], preferred_element_type=F32).astype(BF16)

    tail_copy = remote(kv_tail, kv_got, tail_send, tail_recv, me + 1)

    def q_copy(c):
        return remote(q_tail.at[c], q_got.at[c], q_send.at[c], q_recv.at[c], me + 1)

    tail_of(0)

    @pl.when(me < n - 1)
    def _():
        tail_copy.start()

    for c in range(1, EARLY + 1):
        tail_of(c)

        @pl.when(me < n - 1)
        def _(c=c):
            q_copy(c - 1).start()

    for c in range(EARLY + 1, CHUNKS):
        tail_of(c)

    row = lax.broadcasted_iota(jnp.int32, (SPAN, SPAN), 0)
    column = lax.broadcasted_iota(jnp.int32, (SPAN, SPAN), 1)
    own_clip = seg_ref[pl.ds(me, 1), :]
    clip_column = jnp.sum(jnp.where(row == column, own_clip, 0), axis=1, keepdims=True)
    lane = lax.broadcasted_iota(jnp.int32, (SPAN, HEAD_DIM), 1)
    clips[...] = jnp.where(lane == clip_column, 1.0, 0.0).astype(BF16)
    causal[...] = jnp.where(column <= row, 0.0, LOW)
    clip_row = lax.broadcasted_iota(jnp.int32, (HEAD_DIM, SPAN), 0)
    for slot in range(WINDOW):
        block = me - LAST + slot
        key_clip = seg_ref[pl.ds(jnp.maximum(block, 0), 1), :]
        outside = jnp.where((key_clip == clip_row) & (block >= 0), 0.0, LOW).astype(BF16)
        for g in range(KV_HEADS):
            keys_t[g, HEAD_DIM:, slot * SPAN:(slot + 1) * SPAN] = outside

    @pl.loop(0, me)
    def _(sender):
        count_copy(sender, me).wait_recv()

    device = lax.broadcasted_iota(jnp.int32, counts.shape, 0)
    before = jnp.sum(jnp.where(device < me, counts[...], 0), axis=0)
    lead_in = before[0:1, 0:1] - me * SPAN
    start_row = lax.broadcasted_iota(jnp.int32, (SPAN, 2 * SPAN), 0)
    start_column = lax.broadcasted_iota(jnp.int32, (SPAN, 2 * SPAN), 1)
    shift = jnp.where(start_column + lead_in == start_row + SPAN, 1.0, 0.0).astype(BF16)

    @pl.when(me > 0)
    def _():
        tail_copy.wait_recv()

    def placed(arrived, own):
        both = jnp.concatenate([arrived, own], axis=0)
        return jnp.dot(shift, both, preferred_element_type=F32).astype(BF16)

    window[LAST] = placed(kv_got[...], kv_in[:SPAN])

    def lay_out(slot):
        for g in range(KV_HEADS):
            keys_t[g, :HEAD_DIM, slot * SPAN:(slot + 1) * SPAN] = window[
                slot, :, g * HEAD_DIM:(g + 1) * HEAD_DIM
            ].T
            vals[g, slot * SPAN:(slot + 1) * SPAN, :] = window[
                slot, :, KW + g * HEAD_DIM:KW + (g + 1) * HEAD_DIM
            ]

    lay_out(LAST)

    def block_copy(src, dst, target):
        return remote(window.at[src], window.at[dst], kv_send.at[dst], kv_recv.at[dst], target)

    near = block_copy(LAST, 2, me + 2)
    far = block_copy(LAST, 0, me + 4)
    partner = me + 1 - 2 * core
    beside = (block_copy(LAST, 3, partner), block_copy(2, 3, partner))
    across = (block_copy(2, 1, partner), block_copy(0, 1, partner))

    @pl.when(core == 0)
    def _():
        beside[0].start()

    @pl.when(me + 2 < n)
    def _():
        near.start()

    @pl.when(me + 4 < n)
    def _():
        far.start()

    @pl.when(me < n - 1)
    def _():
        for c in range(EARLY, CHUNKS):
            q_copy(c).start()

    @pl.when(me >= 2)
    def _():
        near.wait_recv()

        @pl.when(core == 0)
        def _():
            across[0].start()

        @pl.when(core == 1)
        def _():
            beside[1].start()

    lay_out(2)

    @pl.when(me >= 4)
    def _():
        far.wait_recv()

        @pl.when(core == 1)
        def _():
            across[1].start()

    lay_out(0)

    @pl.when(me >= 1)
    def _():
        beside[0].wait_recv()

    lay_out(3)

    @pl.when(me >= 3)
    def _():
        across[0].wait_recv()

    lay_out(1)

    scale = math.log2(math.e) / math.sqrt(HEAD_DIM)
    chunks_per_group = CHUNKS // KV_HEADS

    def out_copy(c):
        return pltpu.make_async_copy(
            o_buf.at[c], out.at[:, pl.ds(pl.multiple_of(c * CHUNK, CHUNK), CHUNK)], out_sem.at[c]
        )

    @pl.loop(0, CHUNKS)
    def _(c):
        @pl.when(me > 0)
        def _():
            q_copy(c).wait_recv()

        queries = placed(q_got[c], q_in[c, :SPAN])
        g = c // chunks_per_group
        for h in range(CHUNK_HEADS):
            query = jnp.concatenate([queries[:, h * HEAD_DIM:(h + 1) * HEAD_DIM], clips[...]], axis=1)
            scores = jnp.dot(query, keys_t[g], preferred_element_type=F32)
            past, own = scores[:, :LAST * SPAN], scores[:, LAST * SPAN:] + causal[...]
            peak = jnp.maximum(
                jnp.max(past, axis=1, keepdims=True), jnp.max(own, axis=1, keepdims=True)
            )
            weights = jnp.exp2((jnp.concatenate([past, own], axis=1) - peak) * scale)
            total = jnp.sum(weights, axis=1, keepdims=True)
            summed = jnp.dot(weights.astype(BF16), vals[g], preferred_element_type=F32)
            o_buf[c, :, h * HEAD_DIM:(h + 1) * HEAD_DIM] = (summed / total).astype(BF16)
        out_copy(c).start()

    @pl.loop(0, CHUNKS)
    def _(c):
        out_copy(c).wait()

    @pl.when(me < n - 1)
    def _():
        tail_copy.wait_send()
        for c in range(CHUNKS):
            q_copy(c).wait_send()

    @pl.when(me + 2 < n)
    def _():
        near.wait_send()

    @pl.when(me + 4 < n)
    def _():
        far.wait_send()

    @pl.when(core == 0)
    def _():
        beside[0].wait_send()

        @pl.when(me >= 2)
        def _():
            across[0].wait_send()

    @pl.when(core == 1)
    def _():
        @pl.when(me >= 2)
        def _():
            beside[1].wait_send()

        @pl.when(me >= 4)
        def _():
            across[1].wait_send()

    @pl.loop(me + 1, n)
    def _(target):
        count_copy(me, target).wait_send()


def shards(n, query_frames, key_frames, value_frames, token_counts, segments):
    cap = query_frames.shape[0]
    dma = pltpu.SemaphoreType.DMA
    vmem = pltpu.VMEM
    return pl.pallas_call(
        functools.partial(kernel, n),
        out_shape=jax.ShapeDtypeStruct((SPAN, Q_HEADS * HEAD_DIM), BF16),
        in_specs=[
            pl.BlockSpec(memory_space=pltpu.SMEM),
            pl.BlockSpec(memory_space=pltpu.VMEM),
            pl.BlockSpec(memory_space=pl.ANY),
            pl.BlockSpec(memory_space=pl.ANY),
            pl.BlockSpec(memory_space=pl.ANY),
        ],
        out_specs=pl.BlockSpec(memory_space=pl.ANY),
        scratch_shapes=[
            vmem((n, 8, 128), jnp.int32),
            vmem((CHUNKS, cap, CHUNK), BF16),
            vmem((CHUNKS, SPAN, CHUNK), BF16),
            vmem((CHUNKS, SPAN, CHUNK), BF16),
            vmem((cap, 2 * KW), BF16),
            vmem((SPAN, 2 * KW), BF16),
            vmem((SPAN, 2 * KW), BF16),
            vmem((WINDOW, SPAN, 2 * KW), BF16),
            vmem((KV_HEADS, 2 * HEAD_DIM, WINDOW * SPAN), BF16),
            vmem((KV_HEADS, WINDOW * SPAN, HEAD_DIM), BF16),
            vmem((SPAN, SPAN), F32),
            vmem((SPAN, HEAD_DIM), BF16),
            vmem((CHUNKS, SPAN, CHUNK), BF16),
            dma((CHUNKS,)),
            dma((2,)),
            dma((CHUNKS,)),
            dma((n,)),
            dma((n,)),
            dma,
            dma,
            dma((CHUNKS,)),
            dma((CHUNKS,)),
            dma((WINDOW,)),
            dma((WINDOW,)),
        ],
        compiler_params=pltpu.CompilerParams(collective_id=0, has_side_effects=True),
    )(token_counts, segments.reshape(-1, SPAN), query_frames, key_frames, value_frames)


def solution(mesh):
    in_specs = (
        P(("group", "seq"), None),
        P(("group", "seq"), None),
        P(("group", "seq"), None),
        P(("group", "seq")),
        P("group"),
    )
    out_specs = P(("group", "seq"), None)
    return jax.shard_map(
        functools.partial(shards, mesh.shape["seq"]),
        mesh=mesh, in_specs=in_specs, out_specs=out_specs, check_vma=False,
    )
```

```python
import functools
import math

import jax
import jax.numpy as jnp
from jax import lax
from jax.experimental import pallas as pl
from jax.experimental.pallas import tpu as pltpu
from jax.sharding import PartitionSpec as P

Q_HEADS = 32
KV_HEADS = 4
HEAD_DIM = 128
SPAN = 256
WINDOW = 5
CHUNK_HEADS = 4
CHUNK = CHUNK_HEADS * HEAD_DIM
CHUNKS = Q_HEADS // CHUNK_HEADS
HALF = SPAN // 2
WIDE = WINDOW * SPAN - HALF
KW = KV_HEADS * HEAD_DIM
LAST = WINDOW - 1
LOW = -(2.0**100)
BF16 = jnp.bfloat16
F32 = jnp.float32


def one_hot(rows, columns, shift):
    row = lax.broadcasted_iota(jnp.int32, (rows, columns), 0)
    column = lax.broadcasted_iota(jnp.int32, (rows, columns), 1)
    return jnp.where(column == row + shift, 1.0, 0.0).astype(BF16)


def kernel(
    n, count_ref, seg_ref, qf, kf, vf, out,
    counts, q_in, q_tail, q_got, kv_in, kv_tail, kv_got, window, keys_t, vals, clips, o_buf,
    in_sem, kv_in_sem, out_sem, cnt_send, cnt_recv, tail_send, tail_recv, q_send, q_recv, kv_send, kv_recv,
):
    me = lax.axis_index("seq")
    core = lax.rem(me, 2)
    cap = kv_in.shape[0]

    kv_loads = [
        pltpu.make_async_copy(kf, kv_in.at[:, pl.ds(0, KW)], kv_in_sem.at[0]),
        pltpu.make_async_copy(vf, kv_in.at[:, pl.ds(KW, KW)], kv_in_sem.at[1]),
    ]
    q_loads = [
        pltpu.make_async_copy(qf.at[:, pl.ds(c * CHUNK, CHUNK)], q_in.at[c], in_sem.at[c])
        for c in range(CHUNKS)
    ]
    for load in kv_loads + q_loads:
        load.start()

    count = count_ref[0]
    counts[me] = jnp.full(counts.shape[1:], count, jnp.int32)

    for slot in range(LAST):
        @pl.when(me < LAST - slot)
        def _():
            window[slot] = jnp.zeros(window.shape[1:], BF16)

    @pl.when(me == 0)
    def _():
        kv_got[...] = jnp.zeros_like(kv_got)
        q_got[...] = jnp.zeros_like(q_got)

    barrier = pltpu.get_barrier_semaphore()

    @pl.loop(1, n)
    def _(step):
        pl.semaphore_signal(barrier, inc=1, device_id={"seq": lax.rem(me + step, n)})

    pl.semaphore_wait(barrier, n - 1)

    def remote(src, dst, send, recv, target):
        return pltpu.make_async_remote_copy(
            src_ref=src, dst_ref=dst, send_sem=send, recv_sem=recv, device_id={"seq": target}
        )

    def count_copy(sender, target):
        return remote(counts.at[sender], counts.at[sender], cnt_send.at[target], cnt_recv.at[sender], target)

    @pl.loop(me + 1, n)
    def _(target):
        count_copy(me, target).start()

    for load in kv_loads:
        load.wait()
    ending = one_hot(SPAN, cap, count - SPAN)
    kv_tail[...] = jnp.dot(ending, kv_in[...], preferred_element_type=F32).astype(BF16)

    def tail_of(c):
        q_loads[c].wait()
        q_tail[c] = jnp.dot(ending, q_in[c], preferred_element_type=F32).astype(BF16)

    tail_copy = remote(kv_tail, kv_got, tail_send, tail_recv, me + 1)

    def q_copy(c):
        return remote(q_tail.at[c], q_got.at[c], q_send.at[c], q_recv.at[c], me + 1)

    def clip_row_of(block):
        first = pl.multiple_of(block * SPAN, SPAN)
        return seg_ref[pl.ds(first, SPAN)].reshape(1, SPAN)

    row = lax.broadcasted_iota(jnp.int32, (SPAN, SPAN), 0)
    column = lax.broadcasted_iota(jnp.int32, (SPAN, SPAN), 1)
    own_clip = clip_row_of(me)
    clip_column = jnp.sum(jnp.where(row == column, own_clip, 0), axis=1, keepdims=True)
    lane = lax.broadcasted_iota(jnp.int32, (SPAN, HEAD_DIM), 1)
    clips[...] = jnp.where(lane == clip_column, 1.0, 0.0).astype(BF16)
    clip_row = lax.broadcasted_iota(jnp.int32, (HEAD_DIM, SPAN), 0)
    for slot in range(WINDOW):
        block = me - LAST + slot
        key_clip = clip_row_of(jnp.maximum(block, 0))
        outside = jnp.where((key_clip == clip_row) & (block >= 0), 0.0, LOW).astype(BF16)
        for g in range(KV_HEADS):
            keys_t[g, HEAD_DIM:, slot * SPAN:(slot + 1) * SPAN] = outside
    vals[:, :, HEAD_DIM:] = jnp.ones((KV_HEADS, WINDOW * SPAN, HEAD_DIM), BF16)

    @pl.when(me < n - 1)
    def _():
        tail_copy.start()

    @pl.loop(0, me)
    def _(sender):
        count_copy(sender, me).wait_recv()

    device = lax.broadcasted_iota(jnp.int32, counts.shape, 0)
    before = jnp.sum(jnp.where(device < me, counts[...], 0), axis=0)
    lead_in = before[0:1, 0:1] - me * SPAN
    start_row = lax.broadcasted_iota(jnp.int32, (SPAN, 2 * SPAN), 0)
    start_column = lax.broadcasted_iota(jnp.int32, (SPAN, 2 * SPAN), 1)
    shift = jnp.where(start_column + lead_in == start_row + SPAN, 1.0, 0.0).astype(BF16)

    @pl.when(me > 0)
    def _():
        tail_copy.wait_recv()

    def placed(arrived, own):
        both = jnp.concatenate([arrived, own], axis=0)
        return jnp.dot(shift, both, preferred_element_type=F32).astype(BF16)

    window[LAST] = placed(kv_got[...], kv_in[:SPAN])

    def lay_out(slot):
        for g in range(KV_HEADS):
            keys_t[g, :HEAD_DIM, slot * SPAN:(slot + 1) * SPAN] = window[
                slot, :, g * HEAD_DIM:(g + 1) * HEAD_DIM
            ].T
            vals[g, slot * SPAN:(slot + 1) * SPAN, :HEAD_DIM] = window[
                slot, :, KW + g * HEAD_DIM:KW + (g + 1) * HEAD_DIM
            ]

    lay_out(LAST)

    def block_copy(src, dst, target):
        return remote(window.at[src], window.at[dst], kv_send.at[dst], kv_recv.at[dst], target)

    near = block_copy(LAST, 2, me + 2)
    far = block_copy(LAST, 0, me + 4)
    partner = me + 1 - 2 * core
    beside = (block_copy(LAST, 3, partner), block_copy(2, 3, partner))
    across = (block_copy(2, 1, partner), block_copy(0, 1, partner))

    @pl.when(core == 0)
    def _():
        beside[0].start()

    @pl.when(me + 2 < n)
    def _():
        near.start()

    @pl.when(me + 4 < n)
    def _():
        far.start()

    for c in range(CHUNKS):
        tail_of(c)
        if c > 0:
            @pl.when(me < n - 1)
            def _(c=c):
                q_copy(c - 1).start()

    @pl.when(me < n - 1)
    def _():
        q_copy(CHUNKS - 1).start()

    @pl.when(me >= 2)
    def _():
        near.wait_recv()

        @pl.when(core == 0)
        def _():
            across[0].start()

        @pl.when(core == 1)
        def _():
            beside[1].start()

    lay_out(2)

    @pl.when(me >= 4)
    def _():
        far.wait_recv()

        @pl.when(core == 1)
        def _():
            across[1].start()

    lay_out(0)

    @pl.when(me >= 1)
    def _():
        beside[0].wait_recv()

    lay_out(3)

    @pl.when(me >= 3)
    def _():
        across[0].wait_recv()

    lay_out(1)

    scale = math.log2(math.e) / math.sqrt(HEAD_DIM)
    chunks_per_group = CHUNKS // KV_HEADS
    half_row = lax.broadcasted_iota(jnp.int32, (HALF, HALF), 0)
    half_column = lax.broadcasted_iota(jnp.int32, (HALF, HALF), 1)
    lower = half_column <= half_row

    def out_copy(c):
        return pltpu.make_async_copy(
            o_buf.at[c], out.at[:, pl.ds(pl.multiple_of(c * CHUNK, CHUNK), CHUNK)], out_sem.at[c]
        )

    @pl.loop(0, CHUNKS)
    def _(c):
        @pl.when(me > 0)
        def _():
            q_copy(c).wait_recv()

        queries = placed(q_got[c], q_in[c, :SPAN])
        g = c // chunks_per_group
        for h in range(CHUNK_HEADS):
            columns = slice(h * HEAD_DIM, (h + 1) * HEAD_DIM)
            for part in range(2):
                rows = slice(part * HALF, (part + 1) * HALF)
                reach = slice(part * HALF, part * HALF + WIDE)
                query = jnp.concatenate([queries[rows, columns], clips[rows]], axis=1)
                scores = jnp.dot(query, keys_t[g, :, reach], preferred_element_type=F32)
                ends = jnp.where(lower, scores[:, WIDE - HALF:], scores[:, :HALF])
                middle = scores[:, HALF:WIDE - HALF]
                peak = jnp.maximum(
                    jnp.max(ends, axis=1, keepdims=True), jnp.max(middle, axis=1, keepdims=True)
                )
                end_weights = jnp.exp2((ends - peak) * scale)
                weights = jnp.concatenate(
                    [
                        jnp.where(lower, 0.0, end_weights).astype(BF16),
                        jnp.exp2((middle - peak) * scale).astype(BF16),
                        jnp.where(lower, end_weights, 0.0).astype(BF16),
                    ],
                    axis=1,
                )
                summed = jnp.dot(weights, vals[g, reach, :], preferred_element_type=F32)
                o_buf[c, rows, columns] = (summed[:, :HEAD_DIM] / summed[:, HEAD_DIM:]).astype(BF16)
        out_copy(c).start()

    @pl.loop(0, CHUNKS)
    def _(c):
        out_copy(c).wait()

    @pl.when(me < n - 1)
    def _():
        tail_copy.wait_send()
        for c in range(CHUNKS):
            q_copy(c).wait_send()

    @pl.when(me + 2 < n)
    def _():
        near.wait_send()

    @pl.when(me + 4 < n)
    def _():
        far.wait_send()

    @pl.when(core == 0)
    def _():
        beside[0].wait_send()

        @pl.when(me >= 2)
        def _():
            across[0].wait_send()

    @pl.when(core == 1)
    def _():
        @pl.when(me >= 2)
        def _():
            beside[1].wait_send()

        @pl.when(me >= 4)
        def _():
            across[1].wait_send()

    @pl.loop(me + 1, n)
    def _(target):
        count_copy(me, target).wait_send()


def shards(n, query_frames, key_frames, value_frames, token_counts, segments):
    cap = query_frames.shape[0]
    dma = pltpu.SemaphoreType.DMA
    vmem = pltpu.VMEM
    return pl.pallas_call(
        functools.partial(kernel, n),
        out_shape=jax.ShapeDtypeStruct((SPAN, Q_HEADS * HEAD_DIM), BF16),
        in_specs=[
            pl.BlockSpec(memory_space=pltpu.SMEM),
            pl.BlockSpec(memory_space=pltpu.VMEM),
            pl.BlockSpec(memory_space=pl.ANY),
            pl.BlockSpec(memory_space=pl.ANY),
            pl.BlockSpec(memory_space=pl.ANY),
        ],
        out_specs=pl.BlockSpec(memory_space=pl.ANY),
        scratch_shapes=[
            vmem((n, 8, 128), jnp.int32),
            vmem((CHUNKS, cap, CHUNK), BF16),
            vmem((CHUNKS, SPAN, CHUNK), BF16),
            vmem((CHUNKS, SPAN, CHUNK), BF16),
            vmem((cap, 2 * KW), BF16),
            vmem((SPAN, 2 * KW), BF16),
            vmem((SPAN, 2 * KW), BF16),
            vmem((WINDOW, SPAN, 2 * KW), BF16),
            vmem((KV_HEADS, 2 * HEAD_DIM, WINDOW * SPAN), BF16),
            vmem((KV_HEADS, WINDOW * SPAN, 2 * HEAD_DIM), BF16),
            vmem((SPAN, HEAD_DIM), BF16),
            vmem((CHUNKS, SPAN, CHUNK), BF16),
            dma((CHUNKS,)),
            dma((2,)),
            dma((CHUNKS,)),
            dma((n,)),
            dma((n,)),
            dma,
            dma,
            dma((CHUNKS,)),
            dma((CHUNKS,)),
            dma((WINDOW,)),
            dma((WINDOW,)),
        ],
        compiler_params=pltpu.CompilerParams(collective_id=0, has_side_effects=True),
    )(token_counts, segments, query_frames, key_frames, value_frames)


def solution(mesh):
    in_specs = (
        P(("group", "seq"), None),
        P(("group", "seq"), None),
        P(("group", "seq"), None),
        P(("group", "seq")),
        P("group"),
    )
    out_specs = P(("group", "seq"), None)
    return jax.shard_map(
        functools.partial(shards, mesh.shape["seq"]),
        mesh=mesh, in_specs=in_specs, out_specs=out_specs, check_vma=False,
    )
```
